32 devices in a mesh: groups: 2 (over y), row: 16 (over z, x, core).
Axes of the slice: x: 2, y: 2, z: 4, core: 2. Of those that a mesh axis runs over, the one named last changes fastest.
Arguments:
- raw_samples: bfloat16 [8, 1536, 1280], P('groups', 'row'), parts along dimension 0, may hold values from -64 to 64, as said below
- partner: int32 [32, 3], P(('groups', 'row')), parts along dimension 0, may hold values from -1 to 15, as said below
- counts: int32 [32, 3], P(('groups', 'row')), parts along dimension 0, may hold values from 1 to 4
Outputs:
- correlations: bfloat16 [32, 3, 80, 80, 128], P(('groups', 'row')), parts along dimension 0
The draws below stay inside these ranges and needn't reach their ends.
There are 2 independent parts, one for each index of `groups`. The reference program is written for one: setup_inputs(seed, part) draws one part's arguments, and reference() takes and returns one part's arrays. A program takes and returns all parts, laid end to end along the dimension named above; each array names one. Nothing has to cross between parts.
Inputs may be any that keep to these rules, and one draw needn't show every extreme that they name: `raw_samples`: strain values of each channel and segment at their own scale. `partner`: slot 0 of row i holds i; slots 1 to r hold i + 1 to i + r for some r of 0 to 2 with i + r < 16; the other slots hold -1. Some row has r = 2. A tile stacks its first counts segments.
All inputs are finite; a program needn't handle non-finite values.
Results may differ from the reference program's by a relative error of at most 0.0075.
Values may be sent and summed in bfloat16 or wider, within the bound.
A program may use at most 128 MiB of HBM per device.

```python
import math
import jax
import jax.numpy as jnp
from jax import lax

SEG = 4
SAMPLES = 1536
BINS = 192
FIRST_BIN = 5
LAGS = 128
LAG_STEP = 4
BLOCK = 80
BAND = 2
SLOTS = 3
BLOCKS = 16
CHANNELS = 1280


def draw_raw_samples(key, part):
    first_key, second_key, third_key = jax.random.split(jax.random.fold_in(key, 11), 3)
    shape = (SEG, SAMPLES, CHANNELS)
    seg_scale = jnp.exp(jax.random.uniform(second_key, (SEG, 1, 1), jnp.float32, math.log(0.5), math.log(2.0)))
    chan_scale = jnp.exp(jax.random.uniform(first_key, (1, 1, CHANNELS), jnp.float32, math.log(0.3), math.log(3.0)))
    values = jnp.clip(jax.random.normal(third_key, shape, jnp.float32), -4.0, 4.0)
    return (values * chan_scale * seg_scale).astype(jnp.bfloat16)


def draw_partner(key, part):
    first_key, second_key = jax.random.split(jax.random.fold_in(key, 23))
    block_rows = jnp.arange(BLOCKS, dtype=jnp.int32)
    reaches = jax.random.randint(first_key, (BLOCKS,), 0, BAND + 1, dtype=jnp.int32)
    forced = jax.random.randint(second_key, (), 0, BLOCKS - BAND, dtype=jnp.int32)
    reaches = jnp.where(block_rows == forced, BAND, reaches)
    reaches = jnp.minimum(reaches, BLOCKS - 1 - block_rows)
    offsets = jnp.arange(SLOTS, dtype=jnp.int32)
    listed = jnp.where(offsets[None, :] <= reaches[:, None], block_rows[:, None] + offsets[None, :], -1)
    return listed.astype(jnp.int32)


def with_ends(entries, own_key, low, largest):
    spot = [jax.random.randint(jax.random.fold_in(own_key, axis), (), 0, length) for axis, length in enumerate(entries.shape)]
    main_axis = entries.shape.index(max(entries.shape))
    beside = spot[:main_axis] + [(spot[main_axis] + 1) % entries.shape[main_axis]] + spot[main_axis + 1:]
    return entries.at[tuple(spot)].set(low).at[tuple(beside)].set(largest)


def setup_inputs(seed: int = 0, part: int = 0) -> dict:
    splits = jax.random.split(jax.random.key(seed), 4)
    part_keys = jax.random.split(jax.random.fold_in(splits[3], part), 4)
    raw_samples = draw_raw_samples(jax.random.fold_in(jax.random.fold_in(splits[3], part), 71), part)
    partner = draw_partner(jax.random.fold_in(jax.random.fold_in(splits[3], part), 71), part)
    counts = with_ends(jax.random.randint(part_keys[2], (BLOCKS, SLOTS), 1, SEG + 1), jax.random.fold_in(part_keys[2], 1), 1, SEG).astype(jnp.int32)
    return dict(raw_samples=raw_samples, partner=partner, counts=counts)


def forward_table(length, first_bin, bin_count):
    sample_idx = jnp.arange(length, dtype=jnp.int32)[:, None]
    bin_index = first_bin + jnp.arange(bin_count, dtype=jnp.int32)[None, :]
    angles = 2.0 * math.pi / length * (sample_idx * bin_index % length).astype(jnp.float32)
    return jnp.concatenate([jnp.cos(angles), -jnp.sin(angles)], axis=1).astype(jnp.bfloat16)

def lag_table(length, first_bin, bin_count, lag_count, lag_step):
    bin_index = first_bin + jnp.arange(bin_count, dtype=jnp.int32)[:, None]
    delays = lag_step * (jnp.arange(lag_count, dtype=jnp.int32)[None, :] - lag_count // 2)
    angles = 2.0 * math.pi / length * (bin_index * delays % length).astype(jnp.float32)
    return jnp.concatenate([jnp.cos(angles), -jnp.sin(angles)], axis=0).astype(jnp.bfloat16)

def tile_lags(left_block, right_block, seg_count, lag_matrix):
    segments, block_width, doubled = left_block.shape
    bin_count = doubled // 2
    keep_mask = (jnp.arange(segments, dtype=jnp.int32) < seg_count).astype(jnp.float32)
    left_block = left_block.astype(jnp.float32) * keep_mask[:, None, None]
    right_block = right_block.astype(jnp.float32)
    left_parts = jnp.stack([left_block[..., :bin_count], left_block[..., bin_count:]], axis=1)
    right_parts = jnp.stack([right_block[..., :bin_count], right_block[..., bin_count:]], axis=1)
    turned = jnp.stack([right_block[..., bin_count:], -right_block[..., :bin_count]], axis=1)
    real_sum = jnp.einsum('spaf,spbf->abf', left_parts, right_parts, precision=lax.Precision.HIGHEST)
    imag_sum = jnp.einsum('spaf,spbf->abf', left_parts, turned, precision=lax.Precision.HIGHEST)
    scaling = lax.rsqrt(seg_count.astype(jnp.float32))
    stacked = (jnp.concatenate([real_sum, imag_sum], axis=-1) * scaling).astype(jnp.bfloat16)
    lagged = jnp.dot(stacked.reshape(block_width * block_width, doubled), lag_matrix, preferred_element_type=jnp.float32)
    return lagged.reshape(block_width, block_width, -1) * (1.0 / math.sqrt(bin_count))

def reference(raw_samples, partner, counts):
    segments, length, channels = raw_samples.shape
    blocks = channels // BLOCK
    dft_table = forward_table(length, FIRST_BIN, BINS)
    spectra = jnp.einsum('slc,lf->scf', raw_samples.astype(jnp.float32), dft_table.astype(jnp.float32), precision=lax.Precision.HIGHEST)
    energy = 2.0 * lax.optimization_barrier(jnp.mean(spectra * spectra, axis=-1, keepdims=True))
    white = (spectra * lax.rsqrt(energy + 1e-06)).astype(jnp.bfloat16)
    lag_matrix = lag_table(length, FIRST_BIN, BINS, LAGS, LAG_STEP)
    above_diag = jnp.arange(BLOCK)[:, None] < jnp.arange(BLOCK)[None, :]

    def one_tile(tile_index):
        block_row = tile_index // SLOTS
        offset = tile_index % SLOTS
        partner_block = partner[block_row, offset]
        seg_count = counts[block_row, offset]
        left_block = lax.dynamic_slice_in_dim(white, (block_row * BLOCK).astype(jnp.int32), BLOCK, 1)
        right_block = lax.dynamic_slice_in_dim(white, (jnp.maximum(partner_block, 0) * BLOCK).astype(jnp.int32), BLOCK, 1)
        lagged = tile_lags(left_block, right_block, seg_count, lag_matrix)
        keeping = jnp.where(partner_block == block_row, above_diag, partner_block >= 0)
        return jnp.where(keeping[:, :, None], lagged, 0.0).astype(jnp.bfloat16)
    tiles = lax.map(one_tile, jnp.arange(blocks * SLOTS, dtype=jnp.int32))
    return tiles.reshape(blocks, SLOTS, BLOCK, BLOCK, LAGS)
```

```python
import functools
import math

import jax
import jax.numpy as jnp
import numpy as np
from jax import lax
from jax.experimental import pallas as pl
from jax.experimental.pallas import tpu as pltpu
from jax.sharding import PartitionSpec as P

SAMPLES = 1536
BINS = 192
FIRST_BIN = 5
LAGS = 128
LAG_STEP = 4
SLOTS = 3
WIDTH = 2 * BINS
HALF = BINS - 128
ROWS_PER_STEP = 8


def bin_order():
    bins = np.concatenate([np.arange(BINS), np.arange(128, BINS), np.arange(128)])
    imag = np.arange(WIDTH) >= BINS
    return bins, imag


def angle(product):
    return np.float32(2.0 * math.pi / SAMPLES) * (product % SAMPLES).astype(np.float32)


def forward_table():
    bins, imag = bin_order()
    angles = angle(np.arange(SAMPLES)[:, None] * (FIRST_BIN + bins)[None, :])
    return jnp.asarray(np.where(imag[None, :], -np.sin(angles), np.cos(angles)).astype(np.float32)).astype(jnp.bfloat16)


def lag_tables():
    bins, imag = bin_order()
    delays = LAG_STEP * (np.arange(LAGS) - LAGS // 2)
    angles = angle(delays[:, None] * (FIRST_BIN + bins)[None, :])
    straight = np.cos(angles).astype(np.float32)
    crossed = np.where(imag[None, :], -np.sin(angles), np.sin(angles)).astype(np.float32)
    return jnp.asarray(straight).astype(jnp.bfloat16), jnp.asarray(crossed).astype(jnp.bfloat16)


def from_behind(value, axis, steps):
    count = lax.axis_size(axis)
    initial, last = (max(0, -steps), min(count, count - steps))
    return lax.ppermute(value, axis, [(source, source + steps) for source in range(initial, last)])


def whiten(samples, dft_table):
    spectra = jnp.einsum("slc,lf->scf", samples, dft_table, preferred_element_type=jnp.float32)
    energy = 2.0 * jnp.mean(spectra * spectra, axis=-1, keepdims=True)
    return (spectra * lax.rsqrt(energy + 1e-06)).astype(jnp.bfloat16)


def correlate_kernel(partner, counts, own, near, far, t1, t2, out, right, rows, swapped, w0, w1):
    segments, block, width = own.shape
    step = pl.program_id(0)

    @pl.when(step == 0)
    def _():
        for slot, source in enumerate((own, near, far)):
            seg_count = counts[0, slot]
            for s in range(segments):
                keep = (s < seg_count).astype(jnp.float32)
                right[slot * block:(slot + 1) * block, s * width:(s + 1) * width] = (
                    source[s].astype(jnp.float32) * keep).astype(jnp.bfloat16)
        for s in range(segments):
            value = own[s].astype(jnp.float32)
            rows[s] = value
            swapped[s, :, 0:128] = value[:, 256:384]
            swapped[s, :, 256:384] = value[:, 0:128]
            swapped[s, :, 128:256] = pltpu.roll(value[:, 128:256], HALF, 1)

    buffers = (w0, w1)
    first = pl.multiple_of(step * ROWS_PER_STEP, ROWS_PER_STEP)
    scales = []
    for slot in range(SLOTS):
        live = (partner[0, slot] >= 0).astype(jnp.float32)
        count = jnp.full((8, LAGS), counts[0, slot].astype(jnp.float32), jnp.float32)
        scales.append((lax.rsqrt(count) * (live * (1.0 / math.sqrt(BINS))))[0:1])

    def fill(pair):
        w = buffers[pair % 2]
        for s in range(segments):
            x8 = rows[s, pl.ds(first, ROWS_PER_STEP), :]
            y8 = swapped[s, pl.ds(first, ROWS_PER_STEP), :]
            for k in range(2):
                i = 2 * pair + k
                x = jnp.broadcast_to(x8[i:i + 1], (16, width)).astype(jnp.bfloat16)
                y = jnp.broadcast_to(y8[i:i + 1], (16, width)).astype(jnp.bfloat16)
                for m in range(0, LAGS, 16):
                    w[k * LAGS + m:k * LAGS + m + 16, s * width:(s + 1) * width] = (
                        x * t1[m:m + 16, :] + y * t2[m:m + 16, :])

    pairs = ROWS_PER_STEP // 2
    fill(0)
    for pair in range(pairs):
        if pair + 1 < pairs:
            fill(pair + 1)
        result = lax.dot_general(right[...], buffers[pair % 2][...], (((1,), (1,)), ((), ())),
                                 preferred_element_type=jnp.float32)
        for k in range(2):
            a = first + 2 * pair + k
            part = result[:, k * LAGS:(k + 1) * LAGS]
            for slot in range(SLOTS):
                tile = part[slot * block:(slot + 1) * block] * scales[slot]
                if slot == 0:
                    tile = jnp.where(lax.broadcasted_iota(jnp.int32, tile.shape, 0) > a, tile, 0.0)
                out[0, slot, 2 * pair + k] = tile.astype(jnp.bfloat16)


def correlate(partner, counts, own, near, far):
    segments, block, width = own.shape
    t1, t2 = lag_tables()
    whole = lambda shape: pl.BlockSpec(shape, lambda i, *_: (0,) * len(shape))
    depth = segments * width
    return pl.pallas_call(
        correlate_kernel,
        grid_spec=pltpu.PrefetchScalarGridSpec(
            num_scalar_prefetch=2,
            grid=(block // ROWS_PER_STEP,),
            in_specs=[whole(own.shape)] * 3 + [whole(t1.shape)] * 2,
            out_specs=pl.BlockSpec((1, SLOTS, ROWS_PER_STEP, block, LAGS), lambda i, *_: (0, 0, i, 0, 0)),
            scratch_shapes=[
                pltpu.VMEM((SLOTS * block, depth), jnp.bfloat16),
                pltpu.VMEM(own.shape, jnp.float32),
                pltpu.VMEM(own.shape, jnp.float32),
                pltpu.VMEM((2 * LAGS, depth), jnp.bfloat16),
                pltpu.VMEM((2 * LAGS, depth), jnp.bfloat16),
            ],
        ),
        out_shape=jax.ShapeDtypeStruct((1, SLOTS, block, block, LAGS), jnp.bfloat16),
        cost_estimate=pl.CostEstimate(flops=2 * SLOTS * block * block * LAGS * depth, bytes_accessed=6_000_000, transcendentals=0),
        name="correlate",
    )(partner, counts, own, near, far, t1, t2)


def on_device(raw_samples, partner, counts):
    own = whiten(
        lax.all_to_all(raw_samples, "row", split_axis=2, concat_axis=1, tiled=True), forward_table()
    )
    near = from_behind(own, "row", -1)
    far = from_behind(own, "row", -2)
    return correlate(partner, counts, own, near, far)


def solution(mesh):
    return jax.shard_map(
        on_device,
        mesh=mesh,
        in_specs=(P("groups", "row", None), P(("groups", "row"), None), P(("groups", "row"), None)),
        out_specs=P(("groups", "row"), None, None, None, None),
        check_vma=False,
    )
```

```python
import functools
import math

import jax
import jax.numpy as jnp
import numpy as np
from jax import lax
from jax.experimental import pallas as pl
from jax.experimental.pallas import tpu as pltpu
from jax.sharding import PartitionSpec as P

SAMPLES = 1536
BINS = 192
FIRST_BIN = 5
LAGS = 128
LAG_STEP = 4
SLOTS = 3
WIDTH = 2 * BINS
HALF = BINS - 128
ROWS_PER_STEP = 8
MESH = pl.DeviceIdType.MESH


def bin_order():
    bins = np.concatenate([np.arange(BINS), np.arange(128, BINS), np.arange(128)])
    imag = np.arange(WIDTH) >= BINS
    return bins, imag


def angle(product):
    return np.float32(2.0 * math.pi / SAMPLES) * (product % SAMPLES).astype(np.float32)


def forward_table():
    bins, imag = bin_order()
    angles = angle(np.arange(SAMPLES)[:, None] * (FIRST_BIN + bins)[None, :])
    return jnp.asarray(np.where(imag[None, :], -np.sin(angles), np.cos(angles)).astype(np.float32)).astype(jnp.bfloat16)


def lag_tables():
    bins, imag = bin_order()
    delays = LAG_STEP * (np.arange(LAGS) - LAGS // 2)
    angles = angle(delays[:, None] * (FIRST_BIN + bins)[None, :])
    straight = np.cos(angles).astype(np.float32)
    crossed = np.where(imag[None, :], -np.sin(angles), np.sin(angles)).astype(np.float32)
    return jnp.asarray(straight).astype(jnp.bfloat16), jnp.asarray(crossed).astype(jnp.bfloat16)


def spectra_kernel(n, segments, raw, table, own, near, far, turned, landed, acc, send_sem, recv_sem, pass_send, pass_recv):
    me = lax.axis_index("row")
    block = own.shape[1]
    local = table.shape[1]
    barrier = pltpu.get_barrier_semaphore()

    def ahead(k):
        return lax.rem(me + k, n)

    @pl.loop(1, n)
    def _(k):
        pl.semaphore_signal(barrier, inc=1, device_id={"row": ahead(k)}, device_id_type=MESH)

    @pl.loop(0, raw.shape[1] // 128)
    def _(i):
        part = pl.ds(pl.multiple_of(i * 128, 128), 128)
        turned[part, :] = raw[:, part].T

    pl.semaphore_wait(barrier, n - 1)

    def block_copy(k):
        target = ahead(k)
        return pltpu.make_async_remote_copy(
            src_ref=turned.at[pl.ds(pl.multiple_of(target * block, 16), block)],
            dst_ref=landed.at[me],
            send_sem=send_sem.at[k],
            recv_sem=recv_sem.at[k],
            device_id={"row": target},
            device_id_type=MESH,
        )

    @pl.loop(1, n)
    def _(k):
        block_copy(k).start()

    def transform(x, source):
        stacked = jnp.concatenate([x[:, s * local:(s + 1) * local] for s in range(segments)], axis=0)
        return jnp.dot(stacked, table[source], preferred_element_type=jnp.float32)

    acc[...] = transform(turned[pl.ds(pl.multiple_of(me * block, 16), block), :], me)

    @pl.loop(1, n)
    def _(k):
        block_copy(k).wait_recv()
        source = lax.rem(me + n - k, n)
        acc[...] += transform(landed[source], source)

    spectra = acc[...]
    energy = 2.0 * jnp.mean(spectra * spectra, axis=-1, keepdims=True)
    white = (spectra * lax.rsqrt(energy + 1e-06)).astype(jnp.bfloat16)
    for s in range(segments):
        own[s] = white[s * block:(s + 1) * block]

    def pass_copy(i, target, place):
        return pltpu.make_async_remote_copy(
            src_ref=own, dst_ref=place, send_sem=pass_send.at[i], recv_sem=pass_recv.at[i],
            device_id={"row": target}, device_id_type=MESH,
        )

    for i, place in enumerate((near, far)):
        @pl.when(me >= i + 1)
        def _():
            pass_copy(i, lax.rem(me + n - i - 1, n), place).start()

        @pl.when(me + i + 1 >= n)
        def _():
            place[...] = jnp.zeros_like(place)

    @pl.loop(1, n)
    def _(k):
        block_copy(k).wait_send()

    for i, place in enumerate((near, far)):
        @pl.when(me + i + 1 < n)
        def _():
            pass_copy(i, lax.rem(me + n - i - 1, n), place).wait_recv()

        @pl.when(me >= i + 1)
        def _():
            pass_copy(i, lax.rem(me + n - i - 1, n), place).wait_send()


def white_blocks(raw_samples):
    n = lax.axis_size("row")
    segments, local, channels = raw_samples.shape
    block = channels // n
    white = jax.ShapeDtypeStruct((segments, block, WIDTH), jnp.bfloat16)
    vmem = pl.BlockSpec(memory_space=pltpu.VMEM)
    return pl.pallas_call(
        functools.partial(spectra_kernel, n, segments),
        out_shape=(white,) * 3,
        in_specs=[vmem] * 2,
        out_specs=(vmem,) * 3,
        scratch_shapes=[
            pltpu.VMEM((channels, segments * local), jnp.bfloat16),
            pltpu.VMEM((n, block, segments * local), jnp.bfloat16),
            pltpu.VMEM((segments * block, WIDTH), jnp.float32),
            pltpu.SemaphoreType.DMA((n,)),
            pltpu.SemaphoreType.DMA((n,)),
            pltpu.SemaphoreType.DMA((2,)),
            pltpu.SemaphoreType.DMA((2,)),
        ],
        compiler_params=pltpu.CompilerParams(collective_id=0, has_side_effects=True, vmem_limit_bytes=24 * 2**20),
        name="white_blocks",
    )(raw_samples.reshape(segments * local, channels), forward_table().reshape(n, local, WIDTH))


def correlate_kernel(partner, counts, own, near, far, t1, t2, out, right, rows, swapped, w0, w1):
    segments, block, width = own.shape
    step = pl.program_id(0)

    @pl.when(step == 0)
    def _():
        for slot, source in enumerate((own, near, far)):
            seg_count = counts[0, slot]
            for s in range(segments):
                keep = (s < seg_count).astype(jnp.float32)
                right[slot * block:(slot + 1) * block, s * width:(s + 1) * width] = (
                    source[s].astype(jnp.float32) * keep).astype(jnp.bfloat16)
        for s in range(segments):
            value = own[s].astype(jnp.float32)
            rows[s] = value
            swapped[s, :, 0:128] = value[:, 256:384]
            swapped[s, :, 256:384] = value[:, 0:128]
            swapped[s, :, 128:256] = pltpu.roll(value[:, 128:256], HALF, 1)

    buffers = (w0, w1)
    first = pl.multiple_of(step * ROWS_PER_STEP, ROWS_PER_STEP)
    scales = []
    for slot in range(SLOTS):
        live = (partner[0, slot] >= 0).astype(jnp.float32)
        count = jnp.full((8, LAGS), counts[0, slot].astype(jnp.float32), jnp.float32)
        scales.append((lax.rsqrt(count) * (live * (1.0 / math.sqrt(BINS))))[0:1])

    def fill(pair):
        w = buffers[pair % 2]
        for s in range(segments):
            x8 = rows[s, pl.ds(first, ROWS_PER_STEP), :]
            y8 = swapped[s, pl.ds(first, ROWS_PER_STEP), :]
            for k in range(2):
                i = 2 * pair + k
                x = jnp.broadcast_to(x8[i:i + 1], (16, width)).astype(jnp.bfloat16)
                y = jnp.broadcast_to(y8[i:i + 1], (16, width)).astype(jnp.bfloat16)
                for m in range(0, LAGS, 16):
                    w[k * LAGS + m:k * LAGS + m + 16, s * width:(s + 1) * width] = (
                        x * t1[m:m + 16, :] + y * t2[m:m + 16, :])

    pairs = ROWS_PER_STEP // 2
    fill(0)
    for pair in range(pairs):
        if pair + 1 < pairs:
            fill(pair + 1)
        result = lax.dot_general(right[...], buffers[pair % 2][...], (((1,), (1,)), ((), ())),
                                 preferred_element_type=jnp.float32)
        for k in range(2):
            a = first + 2 * pair + k
            part = result[:, k * LAGS:(k + 1) * LAGS]
            for slot in range(SLOTS):
                tile = part[slot * block:(slot + 1) * block] * scales[slot]
                if slot == 0:
                    tile = jnp.where(lax.broadcasted_iota(jnp.int32, tile.shape, 0) > a, tile, 0.0)
                out[0, slot, 2 * pair + k] = tile.astype(jnp.bfloat16)


def correlate(partner, counts, own, near, far):
    segments, block, width = own.shape
    t1, t2 = lag_tables()
    vmem = pl.BlockSpec(memory_space=pltpu.VMEM)
    depth = segments * width
    return pl.pallas_call(
        correlate_kernel,
        grid_spec=pltpu.PrefetchScalarGridSpec(
            num_scalar_prefetch=2,
            grid=(block // ROWS_PER_STEP,),
            in_specs=[vmem] * 5,
            out_specs=pl.BlockSpec((1, SLOTS, ROWS_PER_STEP, block, LAGS), lambda i, *_: (0, 0, i, 0, 0)),
            scratch_shapes=[
                pltpu.VMEM((SLOTS * block, depth), jnp.bfloat16),
                pltpu.VMEM(own.shape, jnp.float32),
                pltpu.VMEM(own.shape, jnp.float32),
                pltpu.VMEM((2 * LAGS, depth), jnp.bfloat16),
                pltpu.VMEM((2 * LAGS, depth), jnp.bfloat16),
            ],
        ),
        out_shape=jax.ShapeDtypeStruct((1, SLOTS, block, block, LAGS), jnp.bfloat16),
        cost_estimate=pl.CostEstimate(flops=2 * SLOTS * block * block * LAGS * depth, bytes_accessed=6_000_000, transcendentals=0),
        compiler_params=pltpu.CompilerParams(vmem_limit_bytes=20 * 2**20),
        name="correlate",
    )(partner, counts, own, near, far, t1, t2)


def on_device(raw_samples, partner, counts):
    own, near, far = white_blocks(raw_samples)
    return correlate(partner, counts, own, near, far)


def solution(mesh):
    return jax.shard_map(
        on_device,
        mesh=mesh,
        in_specs=(P("groups", "row", None), P(("groups", "row"), None), P(("groups", "row"), None)),
        out_specs=P(("groups", "row"), None, None, None, None),
        check_vma=False,
    )
```

```python
import functools
import math

import jax
import jax.numpy as jnp
import numpy as np
from jax import lax
from jax.experimental import pallas as pl
from jax.experimental.pallas import tpu as pltpu
from jax.sharding import PartitionSpec as P

SAMPLES = 1536
BINS = 192
FIRST_BIN = 5
LAGS = 128
LAG_STEP = 4
SLOTS = 3
WIDTH = 2 * BINS
HALF = BINS - 128
ROWS_PER_STEP = 8
MESH = pl.DeviceIdType.MESH


def bin_order():
    bins = np.concatenate([np.arange(BINS), np.arange(128, BINS), np.arange(128)])
    imag = np.arange(WIDTH) >= BINS
    return bins, imag


def angle(product):
    return np.float32(2.0 * math.pi / SAMPLES) * (product % SAMPLES).astype(np.float32)


def forward_table():
    bins, imag = bin_order()
    angles = angle(np.arange(SAMPLES)[:, None] * (FIRST_BIN + bins)[None, :])
    return jnp.asarray(np.where(imag[None, :], -np.sin(angles), np.cos(angles)).astype(np.float32)).astype(jnp.bfloat16)


def lag_tables():
    bins, imag = bin_order()
    delays = LAG_STEP * (np.arange(LAGS) - LAGS // 2)
    angles = angle(delays[:, None] * (FIRST_BIN + bins)[None, :])
    straight = np.cos(angles).astype(np.float32)
    crossed = np.where(imag[None, :], -np.sin(angles), np.sin(angles)).astype(np.float32)
    return jnp.asarray(straight).astype(jnp.bfloat16), jnp.asarray(crossed).astype(jnp.bfloat16)


def spectra_kernel(n, segments, raw, table, own, near, far, turned, landed, acc, send_sem, recv_sem, pass_send, pass_recv):
    me = lax.axis_index("row")
    block = own.shape[1]
    local = table.shape[1]
    barrier = pltpu.get_barrier_semaphore()

    def ahead(k):
        return lax.rem(me + k, n)

    @pl.loop(1, n)
    def _(k):
        pl.semaphore_signal(barrier, inc=1, device_id={"row": ahead(k)}, device_id_type=MESH)

    @pl.loop(0, raw.shape[1] // 128)
    def _(i):
        part = pl.ds(pl.multiple_of(i * 128, 128), 128)
        turned[part, :] = raw[:, part].T

    pl.semaphore_wait(barrier, n - 1)

    def block_copy(k):
        target = ahead(k)
        return pltpu.make_async_remote_copy(
            src_ref=turned.at[pl.ds(pl.multiple_of(target * block, 16), block)],
            dst_ref=landed.at[me],
            send_sem=send_sem.at[k],
            recv_sem=recv_sem.at[k],
            device_id={"row": target},
            device_id_type=MESH,
        )

    @pl.loop(1, n)
    def _(k):
        block_copy(k).start()

    def transform(x, source):
        stacked = jnp.concatenate([x[:, s * local:(s + 1) * local] for s in range(segments)], axis=0)
        return jnp.dot(stacked, table[source], preferred_element_type=jnp.float32)

    acc[...] = transform(turned[pl.ds(pl.multiple_of(me * block, 16), block), :], me)

    @pl.loop(1, n)
    def _(k):
        block_copy(k).wait_recv()
        source = lax.rem(me + n - k, n)
        acc[...] += transform(landed[source], source)

    spectra = acc[...]
    energy = 2.0 * jnp.mean(spectra * spectra, axis=-1, keepdims=True)
    white = (spectra * lax.rsqrt(energy + 1e-06)).astype(jnp.bfloat16)
    for s in range(segments):
        own[s] = white[s * block:(s + 1) * block]

    def pass_copy(i, target, place):
        return pltpu.make_async_remote_copy(
            src_ref=own, dst_ref=place, send_sem=pass_send.at[i], recv_sem=pass_recv.at[i],
            device_id={"row": target}, device_id_type=MESH,
        )

    for i, place in enumerate((near, far)):
        @pl.when(me >= i + 1)
        def _():
            pass_copy(i, lax.rem(me + n - i - 1, n), place).start()

        @pl.when(me + i + 1 >= n)
        def _():
            place[...] = jnp.zeros_like(place)

    @pl.loop(1, n)
    def _(k):
        block_copy(k).wait_send()

    for i, place in enumerate((near, far)):
        @pl.when(me + i + 1 < n)
        def _():
            pass_copy(i, lax.rem(me + n - i - 1, n), place).wait_recv()

        @pl.when(me >= i + 1)
        def _():
            pass_copy(i, lax.rem(me + n - i - 1, n), place).wait_send()


def white_blocks(raw_samples):
    n = lax.axis_size("row")
    segments, local, channels = raw_samples.shape
    block = channels // n
    white = jax.ShapeDtypeStruct((segments, block, WIDTH), jnp.bfloat16)
    vmem = pl.BlockSpec(memory_space=pltpu.VMEM)
    return pl.pallas_call(
        functools.partial(spectra_kernel, n, segments),
        out_shape=(white,) * 3,
        in_specs=[vmem] * 2,
        out_specs=(vmem,) * 3,
        scratch_shapes=[
            pltpu.VMEM((channels, segments * local), jnp.bfloat16),
            pltpu.VMEM((n, block, segments * local), jnp.bfloat16),
            pltpu.VMEM((segments * block, WIDTH), jnp.float32),
            pltpu.SemaphoreType.DMA((n,)),
            pltpu.SemaphoreType.DMA((n,)),
            pltpu.SemaphoreType.DMA((2,)),
            pltpu.SemaphoreType.DMA((2,)),
        ],
        compiler_params=pltpu.CompilerParams(collective_id=0, has_side_effects=True, vmem_limit_bytes=25000000),
        cost_estimate=pl.CostEstimate(flops=20_000_000_000, bytes_accessed=4_000_000, transcendentals=0),
        name="white_blocks",
    )(raw_samples.reshape(segments * local, channels), forward_table().reshape(n, local, WIDTH))


def correlate_kernel(partner, counts, own, near, far, t1, t2, out, right, rows, swapped, w0, w1):
    segments, block, width = own.shape
    step = pl.program_id(0)

    @pl.when(step == 0)
    def _():
        for slot, source in enumerate((own, near, far)):
            seg_count = counts[0, slot]
            for s in range(segments):
                keep = (s < seg_count).astype(jnp.float32)
                right[slot * block:(slot + 1) * block, s * width:(s + 1) * width] = (
                    source[s].astype(jnp.float32) * keep).astype(jnp.bfloat16)
        for s in range(segments):
            value = own[s].astype(jnp.float32)
            rows[s] = value
            swapped[s, :, 0:128] = value[:, 256:384]
            swapped[s, :, 256:384] = value[:, 0:128]
            swapped[s, :, 128:256] = pltpu.roll(value[:, 128:256], HALF, 1)

    buffers = (w0, w1)
    first = pl.multiple_of(step * ROWS_PER_STEP, ROWS_PER_STEP)
    scales = []
    for slot in range(SLOTS):
        live = (partner[0, slot] >= 0).astype(jnp.float32)
        count = jnp.full((8, LAGS), counts[0, slot].astype(jnp.float32), jnp.float32)
        scales.append((lax.rsqrt(count) * (live * (1.0 / math.sqrt(BINS))))[0:1])

    def fill(pair, base):
        w = buffers[pair % 2]
        for s in range(segments):
            x8 = rows[s, pl.ds(base, ROWS_PER_STEP), :]
            y8 = swapped[s, pl.ds(base, ROWS_PER_STEP), :]
            for k in range(2):
                i = 2 * pair + k
                x = jnp.broadcast_to(x8[i:i + 1], (16, width)).astype(jnp.bfloat16)
                y = jnp.broadcast_to(y8[i:i + 1], (16, width)).astype(jnp.bfloat16)
                for m in range(0, LAGS, 16):
                    w[k * LAGS + m:k * LAGS + m + 16, s * width:(s + 1) * width] = (
                        x * t1[m:m + 16, :] + y * t2[m:m + 16, :])

    pairs = ROWS_PER_STEP // 2
    later = pl.multiple_of(jnp.minimum(first + ROWS_PER_STEP, block - ROWS_PER_STEP), ROWS_PER_STEP)

    @pl.when(step == 0)
    def _():
        fill(0, first)

    for pair in range(pairs):
        if pair + 1 < pairs:
            fill(pair + 1, first)
        else:
            fill(0, later)
        result = lax.dot_general(right[...], buffers[pair % 2][...], (((1,), (1,)), ((), ())),
                                 preferred_element_type=jnp.float32)
        for k in range(2):
            a = first + 2 * pair + k
            part = result[:, k * LAGS:(k + 1) * LAGS]
            for slot in range(SLOTS):
                tile = part[slot * block:(slot + 1) * block] * scales[slot]
                if slot == 0:
                    tile = jnp.where(lax.broadcasted_iota(jnp.int32, tile.shape, 0) > a, tile, 0.0)
                out[0, slot, 2 * pair + k] = tile.astype(jnp.bfloat16)


def correlate(partner, counts, own, near, far):
    segments, block, width = own.shape
    t1, t2 = lag_tables()
    vmem = pl.BlockSpec(memory_space=pltpu.VMEM)
    depth = segments * width
    return pl.pallas_call(
        correlate_kernel,
        grid_spec=pltpu.PrefetchScalarGridSpec(
            num_scalar_prefetch=0,
            grid=(block // ROWS_PER_STEP,),
            in_specs=[pl.BlockSpec(memory_space=pltpu.SMEM)] * 2 + [vmem] * 5,
            out_specs=pl.BlockSpec((1, SLOTS, ROWS_PER_STEP, block, LAGS), lambda i, *_: (0, 0, i, 0, 0)),
            scratch_shapes=[
                pltpu.VMEM((SLOTS * block, depth), jnp.bfloat16),
                pltpu.VMEM(own.shape, jnp.float32),
                pltpu.VMEM(own.shape, jnp.float32),
                pltpu.VMEM((2 * LAGS, depth), jnp.bfloat16),
                pltpu.VMEM((2 * LAGS, depth), jnp.bfloat16),
            ],
        ),
        out_shape=jax.ShapeDtypeStruct((1, SLOTS, block, block, LAGS), jnp.bfloat16),
        cost_estimate=pl.CostEstimate(flops=2 * SLOTS * block * block * LAGS * depth, bytes_accessed=6_000_000, transcendentals=0),
        compiler_params=pltpu.CompilerParams(vmem_limit_bytes=20 * 2**20),
        name="correlate",
    )(partner, counts, own, near, far, t1, t2)


def on_device(raw_samples, partner, counts):
    own, near, far = white_blocks(raw_samples)
    return correlate(partner, counts, own, near, far)


def solution(mesh):
    return jax.shard_map(
        on_device,
        mesh=mesh,
        in_specs=(P("groups", "row", None), P(("groups", "row"), None), P(("groups", "row"), None)),
        out_specs=P(("groups", "row"), None, None, None, None),
        check_vma=False,
    )
```

```python
import functools
import math

import jax
import jax.numpy as jnp
import numpy as np
from jax import lax
from jax.experimental import pallas as pl
from jax.experimental.pallas import tpu as pltpu
from jax.sharding import PartitionSpec as P

SAMPLES = 1536
BINS = 192
FIRST_BIN = 5
LAGS = 128
LAG_STEP = 4
SLOTS = 3
WIDTH = 2 * BINS
HALF = BINS - 128
ROWS_PER_STEP = 16
MESH = pl.DeviceIdType.MESH


def bin_order():
    bins = np.concatenate([np.arange(BINS), np.arange(128, BINS), np.arange(128)])
    imag = np.arange(WIDTH) >= BINS
    return bins, imag


def angle(product):
    return np.float32(2.0 * math.pi / SAMPLES) * (product % SAMPLES).astype(np.float32)


def forward_table():
    bins, imag = bin_order()
    angles = angle(np.arange(SAMPLES)[:, None] * (FIRST_BIN + bins)[None, :])
    return jnp.asarray(np.where(imag[None, :], -np.sin(angles), np.cos(angles)).astype(np.float32)).astype(jnp.bfloat16)


def lag_tables():
    bins, imag = bin_order()
    delays = LAG_STEP * (np.arange(LAGS) - LAGS // 2)
    angles = angle(delays[:, None] * (FIRST_BIN + bins)[None, :])
    straight = np.cos(angles).astype(np.float32)
    crossed = np.where(imag[None, :], -np.sin(angles), np.sin(angles)).astype(np.float32)
    return jnp.asarray(straight).astype(jnp.bfloat16), jnp.asarray(crossed).astype(jnp.bfloat16)


def spectra_kernel(n, segments, raw, table, own, near, far, turned, landed, acc, send_sem, recv_sem, pass_send, pass_recv):
    me = lax.axis_index("row")
    block = own.shape[1]
    local = table.shape[1]
    barrier = pltpu.get_barrier_semaphore()

    def ahead(k):
        return lax.rem(me + k, n)

    @pl.loop(1, n)
    def _(k):
        pl.semaphore_signal(barrier, inc=1, device_id={"row": ahead(k)}, device_id_type=MESH)

    @pl.loop(0, raw.shape[1] // 128)
    def _(i):
        part = pl.ds(pl.multiple_of(i * 128, 128), 128)
        turned[part, :] = raw[:, part].T

    pl.semaphore_wait(barrier, n - 1)

    def block_copy(k):
        target = ahead(k)
        return pltpu.make_async_remote_copy(
            src_ref=turned.at[pl.ds(pl.multiple_of(target * block, 16), block)],
            dst_ref=landed.at[me],
            send_sem=send_sem.at[k],
            recv_sem=recv_sem.at[k],
            device_id={"row": target},
            device_id_type=MESH,
        )

    @pl.loop(1, n)
    def _(k):
        block_copy(k).start()

    def transform(x, source):
        stacked = jnp.concatenate([x[:, s * local:(s + 1) * local] for s in range(segments)], axis=0)
        return jnp.dot(stacked, table[source], preferred_element_type=jnp.float32)

    acc[...] = transform(turned[pl.ds(pl.multiple_of(me * block, 16), block), :], me)

    @pl.loop(1, n)
    def _(k):
        block_copy(k).wait_recv()
        source = lax.rem(me + n - k, n)
        acc[...] += transform(landed[source], source)

    spectra = acc[...]
    energy = 2.0 * jnp.mean(spectra * spectra, axis=-1, keepdims=True)
    white = (spectra * lax.rsqrt(energy + 1e-06)).astype(jnp.bfloat16)
    for s in range(segments):
        own[s] = white[s * block:(s + 1) * block]

    def pass_copy(i, target, place):
        return pltpu.make_async_remote_copy(
            src_ref=own, dst_ref=place, send_sem=pass_send.at[i], recv_sem=pass_recv.at[i],
            device_id={"row": target}, device_id_type=MESH,
        )

    for i, place in enumerate((near, far)):
        @pl.when(me >= i + 1)
        def _():
            pass_copy(i, lax.rem(me + n - i - 1, n), place).start()

        @pl.when(me + i + 1 >= n)
        def _():
            place[...] = jnp.zeros_like(place)

    @pl.loop(1, n)
    def _(k):
        block_copy(k).wait_send()

    for i, place in enumerate((near, far)):
        @pl.when(me + i + 1 < n)
        def _():
            pass_copy(i, lax.rem(me + n - i - 1, n), place).wait_recv()

        @pl.when(me >= i + 1)
        def _():
            pass_copy(i, lax.rem(me + n - i - 1, n), place).wait_send()


def white_blocks(raw_samples):
    n = lax.axis_size("row")
    segments, local, channels = raw_samples.shape
    block = channels // n
    white = jax.ShapeDtypeStruct((segments, block, WIDTH), jnp.bfloat16)
    vmem = pl.BlockSpec(memory_space=pltpu.VMEM)
    return pl.pallas_call(
        functools.partial(spectra_kernel, n, segments),
        out_shape=(white,) * 3,
        in_specs=[vmem] * 2,
        out_specs=(vmem,) * 3,
        scratch_shapes=[
            pltpu.VMEM((channels, segments * local), jnp.bfloat16),
            pltpu.VMEM((n, block, segments * local), jnp.bfloat16),
            pltpu.VMEM((segments * block, WIDTH), jnp.float32),
            pltpu.SemaphoreType.DMA((n,)),
            pltpu.SemaphoreType.DMA((n,)),
            pltpu.SemaphoreType.DMA((2,)),
            pltpu.SemaphoreType.DMA((2,)),
        ],
        compiler_params=pltpu.CompilerParams(collective_id=0, has_side_effects=True, vmem_limit_bytes=25000000),
        cost_estimate=pl.CostEstimate(flops=20_000_000_000, bytes_accessed=4_000_000, transcendentals=0),
        name="white_blocks",
    )(raw_samples.reshape(segments * local, channels), forward_table().reshape(n, local, WIDTH))


def correlate_kernel(partner, counts, own, near, far, t1, t2, out, right, rows, swapped, w0, w1):
    segments, block, width = own.shape
    step = pl.program_id(0)

    @pl.when(step == 0)
    def _():
        for slot, source in enumerate((own, near, far)):
            seg_count = counts[0, slot]
            for s in range(segments):
                keep = (s < seg_count).astype(jnp.float32)
                right[slot * block:(slot + 1) * block, s * width:(s + 1) * width] = (
                    source[s].astype(jnp.float32) * keep).astype(jnp.bfloat16)
        for s in range(segments):
            value = own[s].astype(jnp.float32)
            rows[s] = value
            swapped[s, :, 0:128] = value[:, 256:384]
            swapped[s, :, 256:384] = value[:, 0:128]
            swapped[s, :, 128:256] = pltpu.roll(value[:, 128:256], HALF, 1)

    buffers = (w0, w1)
    first = pl.multiple_of(step * ROWS_PER_STEP, ROWS_PER_STEP)
    scales = []
    for slot in range(SLOTS):
        live = (partner[0, slot] >= 0).astype(jnp.float32)
        count = jnp.full((8, LAGS), counts[0, slot].astype(jnp.float32), jnp.float32)
        scales.append((lax.rsqrt(count) * (live * (1.0 / math.sqrt(BINS))))[0:1])

    def fill(pair, base):
        w = buffers[pair % 2]
        for s in range(segments):
            x8 = rows[s, pl.ds(base, ROWS_PER_STEP), :]
            y8 = swapped[s, pl.ds(base, ROWS_PER_STEP), :]
            for k in range(2):
                i = 2 * pair + k
                x = jnp.broadcast_to(x8[i:i + 1], (16, width)).astype(jnp.bfloat16)
                y = jnp.broadcast_to(y8[i:i + 1], (16, width)).astype(jnp.bfloat16)
                for m in range(0, LAGS, 16):
                    w[k * LAGS + m:k * LAGS + m + 16, s * width:(s + 1) * width] = (
                        x * t1[m:m + 16, :] + y * t2[m:m + 16, :])

    pairs = ROWS_PER_STEP // 2
    later = pl.multiple_of(jnp.minimum(first + ROWS_PER_STEP, block - ROWS_PER_STEP), ROWS_PER_STEP)

    @pl.when(step == 0)
    def _():
        fill(0, first)

    for pair in range(pairs):
        if pair + 1 < pairs:
            fill(pair + 1, first)
        else:
            fill(0, later)
        result = lax.dot_general(right[...], buffers[pair % 2][...], (((1,), (1,)), ((), ())),
                                 preferred_element_type=jnp.float32)
        for k in range(2):
            a = first + 2 * pair + k
            part = result[:, k * LAGS:(k + 1) * LAGS]
            for slot in range(SLOTS):
                tile = part[slot * block:(slot + 1) * block] * scales[slot]
                if slot == 0:
                    tile = jnp.where(lax.broadcasted_iota(jnp.int32, tile.shape, 0) > a, tile, 0.0)
                out[0, slot, 2 * pair + k] = tile.astype(jnp.bfloat16)


def correlate(partner, counts, own, near, far):
    segments, block, width = own.shape
    t1, t2 = lag_tables()
    vmem = pl.BlockSpec(memory_space=pltpu.VMEM)
    depth = segments * width
    return pl.pallas_call(
        correlate_kernel,
        grid_spec=pltpu.PrefetchScalarGridSpec(
            num_scalar_prefetch=0,
            grid=(block // ROWS_PER_STEP,),
            in_specs=[pl.BlockSpec(memory_space=pltpu.SMEM)] * 2 + [vmem] * 5,
            out_specs=pl.BlockSpec((1, SLOTS, ROWS_PER_STEP, block, LAGS), lambda i, *_: (0, 0, i, 0, 0)),
            scratch_shapes=[
                pltpu.VMEM((SLOTS * block, depth), jnp.bfloat16),
                pltpu.VMEM(own.shape, jnp.float32),
                pltpu.VMEM(own.shape, jnp.float32),
                pltpu.VMEM((2 * LAGS, depth), jnp.bfloat16),
                pltpu.VMEM((2 * LAGS, depth), jnp.bfloat16),
            ],
        ),
        out_shape=jax.ShapeDtypeStruct((1, SLOTS, block, block, LAGS), jnp.bfloat16),
        cost_estimate=pl.CostEstimate(flops=2 * SLOTS * block * block * LAGS * depth, bytes_accessed=6_000_000, transcendentals=0),
        compiler_params=pltpu.CompilerParams(vmem_limit_bytes=20 * 2**20),
        name="correlate",
    )(partner, counts, own, near, far, t1, t2)


def on_device(raw_samples, partner, counts):
    own, near, far = white_blocks(raw_samples)
    return correlate(partner, counts, own, near, far)


def solution(mesh):
    return jax.shard_map(
        on_device,
        mesh=mesh,
        in_specs=(P("groups", "row", None), P(("groups", "row"), None), P(("groups", "row"), None)),
        out_specs=P(("groups", "row"), None, None, None, None),
        check_vma=False,
    )
```
